32 devices in a mesh: gx: 16 (over z, y, core), gy: 2 (over x).
Axes of the slice: x: 2, y: 2, z: 4, core: 2. Of those that a mesh axis runs over, the one named last changes fastest.
Arguments:
- old_block: float32 [12288, 24576], P('gx', 'gy'), may hold values from -6 to 6
- vectors: bfloat16 [256, 2, 12288], P(None, 'gy', 'gx'), may hold values from -4 to 4
- prior: bfloat16 [32768, 3072], P('gx', 'gy'), may hold values from -2 to 2
- pair_columns: float32 [32768, 128], P(('gx', 'gy')), may hold values from -6 to 6
- pivots: int32 [128], replicated, may hold values from 0 to 32767
Outputs:
- new_block: float32 [12288, 24576], P('gx', 'gy')
- residual_columns: float32 [32768, 128], P(('gx', 'gy'))
The draws below stay inside these ranges and needn't reach their ends.
Inputs may be any that keep to these rules, and one draw needn't show every extreme that they name: `pivots`: pivot AO-pair row indices, repeats possible.
All inputs are finite; a program needn't handle non-finite values.
Results may differ from the reference program's by a relative error of at most 0.0055.
Values may be sent and summed in bfloat16 or wider, within the bound.
No kernel may reach another device: no remote copies, remote signals or barrier semaphores. Data moves between devices by JAX's collectives and lax.ppermute only.
A program may use at most 192 MiB of HBM per device.

```python
import jax
import jax.numpy as jnp
from jax import lax

NVEC = 256
NPRIOR = 3072
NPIV = 128
NIA = 24576
SLAB = 12288
NPAIR = 32768
N_GY = 2


def plant(entries, stream_key, low, largest):
    longest = entries.shape.index(max(entries.shape))
    spots = []
    for shift in (0, 1):
        where = [jax.random.randint(jax.random.fold_in(stream_key, axis), (), 0, length) for axis, length in enumerate(entries.shape)]
        where[longest] = (where[longest] + shift) % entries.shape[longest]
        spots.append(tuple(where))
    return entries.at[spots[0]].set(low).at[spots[1]].set(largest)


def block_levels(own_key, extent, split, least, largest):
    level = 1.0
    for axis_at, shards_of in split:
        steps = jax.random.uniform(jax.random.fold_in(jax.random.fold_in(own_key, 6), axis_at), (shards_of,), jnp.float32, least / len(split), largest / len(split))
        level = level * jnp.repeat(jnp.exp(steps), extent[axis_at] // shards_of).reshape((-1,) + (1,) * (len(extent) - 1 - axis_at))
    return level


def scatter_about(own_key, extent, deviation, bound, split=(), held_as=jnp.bfloat16):
    drawn = jax.random.normal(own_key, extent, jnp.float32) * deviation
    if len(split) > 0:
        drawn = block_levels(own_key, extent, split, -0.22, 0.18) * drawn
    return jnp.clip(drawn, min=-bound, max=bound).astype(held_as)


def setup_inputs(seed: int = 0) -> dict:
    streams_of = jax.random.split(jax.random.key(seed), 6)
    old_block = scatter_about(streams_of[0], (SLAB, NIA), 1.0, 6.0, ((0, 16), (1, 2)), jnp.float32)
    vectors = scatter_about(streams_of[1], (NVEC, N_GY, NIA // N_GY), (NVEC ** -0.25), 4.0, ((1, 2), (2, 16)))
    prior = scatter_about(streams_of[2], (NPAIR, NPRIOR), (NPRIOR ** -0.25), 2.0, ((0, 16), (1, 2)))
    pair_columns = scatter_about(streams_of[3], (NPAIR, NPIV), 1.0, 6.0, ((0, 32),), jnp.float32)
    pivots = plant(jax.random.randint(streams_of[4], (NPIV,), 0, NPAIR), jax.random.fold_in(streams_of[4], 1), 0, NPAIR - 1).astype(jnp.int32)
    return dict(old_block=old_block, vectors=vectors, prior=prior, pair_columns=pair_columns, pivots=pivots)


def reference(old_block, vectors, prior, pair_columns, pivots):
    flat = vectors.reshape(NVEC, NIA)
    slab = NIA // N_GY
    new_block = old_block + jnp.dot(flat[:, :slab].T, flat, preferred_element_type=jnp.float32)
    picked = jnp.take(prior, pivots, axis=0)
    width = NPRIOR // N_GY
    intersection = jnp.zeros((prior.shape[0], NPIV), jnp.float32)
    for group in range(N_GY):
        part = jnp.dot(prior[:, group * width:(group + 1) * width], picked[:, group * width:(group + 1) * width].T, preferred_element_type=jnp.float32)
        rounded = lax.optimization_barrier(part.astype(jnp.bfloat16))
        intersection = intersection + rounded.astype(jnp.float32)
    return new_block, pair_columns - intersection
```

```python
import functools

import jax
import jax.numpy as jnp
from jax import lax
from jax.experimental import pallas as pl
from jax.experimental.pallas import tpu as pltpu
from jax.sharding import PartitionSpec as P


def factors(n):
    core = 2 if n % 2 == 0 else 1
    near = 2 if (n // core) % 2 == 0 else 1
    return n // (core * near), near, core


HBM = pl.BlockSpec(memory_space=pltpu.HBM)
VMEM = pl.BlockSpec(memory_space=pltpu.VMEM)
SMEM = pl.BlockSpec(memory_space=pltpu.SMEM)


def keep(x):
    return pltpu.with_memory_space_constraint(x, pltpu.HBM)


def call(kernel, out_shape, operands, specs, out_specs, scratch=(), aliases=None, limit=8, flops=0):
    return pl.pallas_call(
        kernel,
        out_shape=out_shape,
        in_specs=specs,
        out_specs=out_specs,
        scratch_shapes=list(scratch),
        input_output_aliases=aliases or {},
        compiler_params=pltpu.CompilerParams(vmem_limit_bytes=limit * 1024 * 1024),
        cost_estimate=pl.CostEstimate(flops=flops, bytes_accessed=0, transcendentals=0),
    )(*operands)


def update_kernel(me, *rest, spots, extent, tiles, first):
    far, near, cores = extent
    count = len(spots)
    held, arrive, leave = rest[-3:]
    high, width = held.shape[1:]
    z, y, c = me[0] // (near * cores), me[0] // cores % near, me[0] % cores
    pieces = [(at, tile) for at in range(count) for tile in range(tiles)]
    if first:
        mask, own, got, *blocks = rest[: count + 2]
        old, out, slab, mine, here = rest[count + 2 : count + 7]
        blocks = [mine, *blocks]
    else:
        slab, *blocks = rest[: count + 1]
        old, out = rest[count + 1], rest[-4]

    def spot(at, tile):
        a, b, d = spots[at]
        column = (((z + a + far) % far * near) + (y + b) % near) * cores + (c + d) % cores
        return pl.ds(tile * high, high), pl.ds(pl.multiple_of(column * width, 128), width)

    def load(n):
        return pltpu.make_async_copy(old.at[spot(*pieces[n])], held.at[n], arrive.at[n])

    def save(n):
        return pltpu.make_async_copy(held.at[n], out.at[spot(*pieces[n])], leave.at[n])

    if first:
        bring = pltpu.make_async_copy(own, mine, here)
        bring.start()
    for n in range(len(pieces)):
        load(n).start()
    if first:
        bring.wait()
        chosen = jnp.where(mask[0] != 0, got[...].astype(jnp.float32), mine[...].astype(jnp.float32))
        slab[...] = chosen.T.astype(slab.dtype)
    for n, (at, tile) in enumerate(pieces):
        load(n).wait()
        held[n] += jnp.dot(
            slab[tile * high : (tile + 1) * high, :], blocks[at][...], preferred_element_type=jnp.float32
        )
        save(n).start()
    for n in range(len(pieces)):
        save(n).wait()


def update(me, rows_of, old, blocks, spots, extent, target):
    first = target is None
    inner, width = blocks[-1].shape
    rows = old.shape[0]
    count = len(blocks)
    tiles = next(t for t in (3, 2, 1) if rows % (8 * t) == 0)
    high = rows // tiles
    shape = jax.ShapeDtypeStruct(old.shape, old.dtype)
    scratch = [
        pltpu.VMEM((count * tiles, high, width), old.dtype),
        pltpu.SemaphoreType.DMA((count * tiles,)),
        pltpu.SemaphoreType.DMA((count * tiles,)),
    ]
    if first:
        mask, got = rows_of
        operands = [me, mask, keep(blocks[0]), got, *blocks[1:], keep(old)]
        specs = [SMEM, SMEM, HBM, VMEM] + [VMEM] * (count - 1) + [HBM]
        aliases = {}
        outs = [shape, jax.ShapeDtypeStruct((rows, inner), got.dtype)]
        out_specs = [HBM, VMEM]
        scratch = [pltpu.VMEM((inner, width), got.dtype), pltpu.SemaphoreType.DMA] + scratch
    else:
        operands = [me, rows_of, *blocks, keep(old), target]
        specs = [SMEM, VMEM] + [VMEM] * count + [HBM, HBM]
        aliases = {len(operands) - 1: 0}
        outs, out_specs = shape, HBM
    return call(
        functools.partial(update_kernel, spots=spots, extent=extent, tiles=tiles, first=first),
        outs,
        operands,
        specs,
        out_specs,
        scratch=scratch,
        aliases=aliases,
        limit=16,
        flops=2 * rows * inner * width * count,
    )


def add_kernel(a, b, out):
    out[...] = a[...] + b[...]


def add(a, b):
    return call(add_kernel, jax.ShapeDtypeStruct(a.shape, a.dtype), [a, b], [VMEM, VMEM], VMEM)


def pick_kernel(pivots, me, prior, kept, sent, tiles, total, owned, spots, arrive, *, cores):
    count = pivots.shape[0]
    rows = prior.shape[0]
    base = me[0] * rows

    def list_owned(k, found):
        row = pivots[k] - base
        owned[found] = k
        spots[found] = row
        return found + jnp.where(jnp.logical_and(row >= 0, row < rows), 1, 0)

    found = lax.fori_loop(0, count, list_owned, 0, unroll=8)

    def copy(n):
        start = pl.multiple_of(spots[n] // 8 * 8, 8)
        return pltpu.make_async_copy(prior.at[pl.ds(start, 8), :], tiles.at[n], arrive)

    def begin(n, carry):
        copy(n).start()
        return carry

    lax.fori_loop(0, found, begin, 0)
    total[...] = jnp.zeros_like(total)

    def finish(n, carry):
        copy(n).wait()
        return carry

    lax.fori_loop(0, found, finish, 0)

    def place(n, carry):
        tile = tiles[n].astype(jnp.float32)
        at = lax.broadcasted_iota(jnp.int32, tile.shape, 0)
        row = jnp.sum(jnp.where(at == spots[n] % 8, tile, 0.0), axis=0, keepdims=True)
        total[pl.ds(owned[n], 1), :] = row
        return carry

    lax.fori_loop(0, found, place, 0)
    half = count // cores
    c = me[0] % cores
    kept[...] = total[pl.ds(pl.multiple_of(c * half, 8), half), :].astype(kept.dtype)
    if cores > 1:
        sent[...] = total[pl.ds(pl.multiple_of((1 - c) * half, 8), half), :].astype(sent.dtype)


def pick(pivots, me, prior, cores):
    count = pivots.shape[0]
    width = prior.shape[1]
    shape = jax.ShapeDtypeStruct((count // cores, width), prior.dtype)
    return call(
        functools.partial(pick_kernel, cores=cores),
        [shape, shape],
        [pivots, me, keep(prior)],
        [SMEM, SMEM, HBM],
        [VMEM, VMEM],
        scratch=[
            pltpu.VMEM((count, 8, width), prior.dtype),
            pltpu.VMEM((count, width), jnp.float32),
            pltpu.SMEM((count + 8,), jnp.int32),
            pltpu.SMEM((count + 8,), jnp.int32),
            pltpu.SemaphoreType.DMA,
        ],
        limit=5,
    )


def parts_kernel(me, mine, *rest, cores, groups):
    prior, kept = rest[0], rest[1]
    outs = rest[1 + cores : 1 + cores + groups]
    picked = rest[-1]
    height = outs[0].shape[0]
    half = kept.shape[0]
    c = me[0] % cores
    picked[pl.ds(pl.multiple_of(c * half, 8), half), :] = kept[...]
    if cores > 1:
        picked[pl.ds(pl.multiple_of((1 - c) * half, 8), half), :] = rest[2][...]
    for g in range(groups):
        start = (mine[0] + 1 + g) % groups * height
        outs[g][...] = lax.dot_general(
            prior[pl.ds(pl.multiple_of(start, 8), height), :],
            picked[...],
            (((1,), (1,)), ((), ())),
            preferred_element_type=jnp.float32,
        ).astype(outs[g].dtype)


def parts_of(me, mine, prior, picked, cores, groups):
    rows, width = prior.shape
    count = picked[0].shape[0] * cores
    height = rows // groups
    return call(
        functools.partial(parts_kernel, cores=cores, groups=groups),
        [jax.ShapeDtypeStruct((height, count), prior.dtype)] * groups,
        [me, mine, prior, *picked],
        [SMEM, SMEM, VMEM] + [VMEM] * cores,
        [VMEM] * groups,
        scratch=[pltpu.VMEM((count, width), prior.dtype)],
        limit=16,
    )


def local(old_block, vectors, prior, pair_columns, pivots):
    size = lax.axis_size("gx")
    groups = lax.axis_size("gy")
    far, near, cores = factors(size)
    me = lax.axis_index("gx")
    mine = lax.axis_index("gy")
    everyone = [(a, b, d) for a in range(far) for b in range(near) for d in range(cores)]

    def place(a, b, d):
        return (a % far * near + b % near) * cores + d % cores

    def shift(x, a=0, b=0, d=0):
        return lax.ppermute(x, "gx", [(place(i, j, k), place(i + a, j + b, k + d)) for i, j, k in everyone])

    def swap_far(x, bit):
        return lax.ppermute(x, "gx", [(place(i, j, k), place(i ^ bit, j, k)) for i, j, k in everyone])

    own = vectors.reshape(vectors.shape[0], vectors.shape[2])
    width = own.shape[1]
    tiled = width % 128 == 0

    lines = [(own, 0)]
    forward = backward = own
    if tiled:
        for step in range(1, far // 2 + 1):
            forward = shift(forward, a=1)
            lines.append((forward, -step))
            if step < far - far // 2:
                backward = shift(backward, a=-1)
                lines.append((backward, step))

    slab = own
    reach = 1
    while reach < groups:
        got = lax.ppermute(slab, "gy", [(g, g + reach) for g in range(reach) if g + reach < groups])
        takes = jnp.logical_and(mine >= reach, mine < 2 * reach)
        reach *= 2
        if reach < groups:
            slab = jnp.where(takes, got, slab)
    if groups == 1:
        got, takes = own, mine > 0

    kept, sent = pick(pivots, me[None], prior, cores)

    if tiled:
        blocks, spots = {}, {}
        for line, (block, away) in enumerate(lines):
            at = line * near * cores
            blocks[at] = block
            for e in range(near):
                for f in range(cores):
                    spots[at + e * cores + f] = (away, e, f)
            if cores > 1:
                blocks[at + 1] = shift(block, d=1)
            if near > 1:
                blocks[at + cores] = shift(block, b=1)
                if cores > 1:
                    blocks[at + cores + 1] = shift(blocks[at + cores], d=1)
        new_block = None
        rows_of = (takes.astype(jnp.int32)[None], got)
        for number, batch in enumerate(batches(far, near, cores)):
            new_block = update(
                me[None],
                rows_of,
                old_block,
                [blocks[at] for at in batch],
                [spots[at] for at in batch],
                (far, near, cores),
                new_block,
            )
            if number == 0:
                new_block, rows_of = new_block
    else:
        every = lax.all_gather(own, "gx", axis=1, tiled=True)
        slab = jnp.where(takes, got, slab)
        new_block = old_block + jnp.dot(slab.T, every, preferred_element_type=jnp.float32)

    if cores > 1:
        kept = add(kept, shift(sent, d=1))
    if near > 1:
        kept = add(kept, shift(kept, b=1))
    bit = 1
    while bit < far:
        kept = add(kept, swap_far(kept, bit))
        bit *= 2
    picked = [kept]
    if cores > 1:
        picked.append(shift(kept, d=1))

    parts = parts_of(me[None], mine[None], prior, picked, cores, groups)
    total = parts[-1].astype(jnp.float32)
    for step in range(1, groups):
        got = lax.ppermute(parts[step - 1], "gy", [(g, (g + step) % groups) for g in range(groups)])
        total = total + got.astype(jnp.float32)
    return new_block, pair_columns - total


def batches(far, near, cores):
    if (far, near, cores) == (4, 2, 2):
        return [[0, 1, 2, 3], [4, 5, 8, 9], [6, 7, 12, 13], [10, 11, 14, 15]]
    return [list(range(at, at + near * cores)) for at in range(0, far * near * cores, near * cores)]


def solution(mesh):
    placed = (P("gx", "gy"), P(None, "gy", "gx"), P("gx", "gy"), P(("gx", "gy"), None), P())

    return jax.shard_map(
        local,
        mesh=mesh,
        in_specs=placed,
        out_specs=(P("gx", "gy"), P(("gx", "gy"), None)),
        check_vma=False,
    )
```

```python
import functools

import jax
import jax.numpy as jnp
from jax import lax
from jax.experimental import pallas as pl
from jax.experimental.pallas import tpu as pltpu
from jax.sharding import PartitionSpec as P


def factors(n):
    core = 2 if n % 2 == 0 else 1
    near = 2 if (n // core) % 2 == 0 else 1
    return n // (core * near), near, core


HBM = pl.BlockSpec(memory_space=pltpu.HBM)
VMEM = pl.BlockSpec(memory_space=pltpu.VMEM)
SMEM = pl.BlockSpec(memory_space=pltpu.SMEM)


def keep(x):
    return pltpu.with_memory_space_constraint(x, pltpu.HBM)


def call(kernel, out_shape, operands, specs, out_specs, scratch=(), aliases=None, limit=8, flops=0):
    return pl.pallas_call(
        kernel,
        out_shape=out_shape,
        in_specs=specs,
        out_specs=out_specs,
        scratch_shapes=list(scratch),
        input_output_aliases=aliases or {},
        compiler_params=pltpu.CompilerParams(vmem_limit_bytes=limit * 1024 * 1024),
        cost_estimate=pl.CostEstimate(flops=flops, bytes_accessed=0, transcendentals=0),
    )(*operands)


def update_kernel(me, *rest, spots, extent, tiles, first, tail):
    far, near, cores = extent
    count = len(spots)
    if tail:
        rest, (total, pair_in, pair_out) = rest[:-3], rest[-3:]
    held, arrive, leave = rest[-3:]
    high, width = held.shape[1:]
    z, y, c = me[0] // (near * cores), me[0] // cores % near, me[0] % cores
    pieces = [(at, tile) for at in range(count) for tile in range(tiles)]
    lag = 3 if len(pieces) >= 8 else 0
    if first:
        mask, own, got, *blocks = rest[: count + 2]
        old, out, slab, mine, here = rest[count + 2 : count + 7]
        blocks = [mine, *blocks]
    else:
        slab, *blocks = rest[: count + 1]
        old = rest[count + 1]
        pair, *parts = rest[count + 3 : count + 3 + tail] if tail else [None]
        out = rest[count + 3 + tail]

    def spot(at, tile):
        a, b, d = spots[at]
        column = (((z + a + far) % far * near) + (y + b) % near) * cores + (c + d) % cores
        return pl.ds(tile * high, high), pl.ds(pl.multiple_of(column * width, 128), width)

    def load(n):
        return pltpu.make_async_copy(old.at[spot(*pieces[n])], held.at[n], arrive.at[n])

    def save(n):
        return pltpu.make_async_copy(held.at[n], out.at[spot(*pieces[n])], leave.at[n])

    if first:
        bring = pltpu.make_async_copy(own, mine, here)
        bring.start()
    for n in range(len(pieces)):
        load(n).start()
    if tail:
        residual = rest[count + 4 + tail]
        pair_load = pltpu.make_async_copy(pair, total, pair_in)
        pair_save = pltpu.make_async_copy(total, residual, pair_out)
        pair_load.start()
    if first:
        bring.wait()
        chosen = jnp.where(mask[0] != 0, got[...].astype(jnp.float32), mine[...].astype(jnp.float32))
        slab[...] = chosen.T.astype(slab.dtype)
    for n, (at, tile) in enumerate(pieces):
        load(n).wait()
        held[n] += jnp.dot(
            slab[tile * high : (tile + 1) * high, :], blocks[at][...], preferred_element_type=jnp.float32
        )
        if n >= lag:
            save(n - lag).start()
    if tail:
        pair_load.wait()
        gathered = parts[0][...].astype(jnp.float32)
        for part in parts[1:]:
            gathered = gathered + part[...].astype(jnp.float32)
        total[...] -= gathered
        pair_save.start()
    for n in range(len(pieces) - lag, len(pieces)):
        save(n).start()
    if tail:
        pair_save.wait()
    for n in range(len(pieces)):
        save(n).wait()


def update(me, rows_of, old, blocks, spots, extent, target, tail=()):
    first = target is None
    inner, width = blocks[-1].shape
    rows = old.shape[0]
    count = len(blocks)
    tiles = next(t for t in (2, 1) if rows % (8 * t) == 0)
    high = rows // tiles
    shape = jax.ShapeDtypeStruct(old.shape, old.dtype)
    scratch = [
        pltpu.VMEM((count * tiles, high, width), old.dtype),
        pltpu.SemaphoreType.DMA((count * tiles,)),
        pltpu.SemaphoreType.DMA((count * tiles,)),
    ]
    if first:
        mask, got = rows_of
        operands = [me, mask, keep(blocks[0]), got, *blocks[1:], keep(old)]
        specs = [SMEM, SMEM, HBM, VMEM] + [VMEM] * (count - 1) + [HBM]
        aliases = {}
        outs = [shape, jax.ShapeDtypeStruct((rows, inner), got.dtype)]
        out_specs = [HBM, VMEM]
        scratch = [pltpu.VMEM((inner, width), got.dtype), pltpu.SemaphoreType.DMA] + scratch
    else:
        operands = [me, rows_of, *blocks, keep(old), target]
        specs = [SMEM, VMEM] + [VMEM] * count + [HBM, HBM]
        aliases = {len(operands) - 1: 0}
        outs, out_specs = [shape], [HBM]
        if tail:
            operands += [keep(tail[0]), *tail[1:]]
            specs += [HBM] + [VMEM] * (len(tail) - 1)
            outs.append(jax.ShapeDtypeStruct(tail[0].shape, tail[0].dtype))
            out_specs.append(HBM)
            scratch += [
                pltpu.VMEM(tail[0].shape, tail[0].dtype),
                pltpu.SemaphoreType.DMA,
                pltpu.SemaphoreType.DMA,
            ]
    return call(
        functools.partial(update_kernel, spots=spots, extent=extent, tiles=tiles, first=first, tail=len(tail)),
        outs,
        operands,
        specs,
        out_specs,
        scratch=scratch,
        aliases=aliases,
        limit=16,
        flops=2 * rows * inner * width * count,
    )


def add_kernel(a, b, out):
    out[...] = a[...] + b[...]


def add(a, b):
    return call(add_kernel, jax.ShapeDtypeStruct(a.shape, a.dtype), [a, b], [VMEM, VMEM], VMEM)


def pick_kernel(pivots, me, prior, kept, sent, tiles, total, owned, spots, arrive, *, cores):
    count = pivots.shape[0]
    rows = prior.shape[0]
    base = me[0] * rows

    def list_owned(k, found):
        row = pivots[k] - base
        owned[found] = k
        spots[found] = row
        return found + jnp.where(jnp.logical_and(row >= 0, row < rows), 1, 0)

    found = lax.fori_loop(0, count, list_owned, 0, unroll=8)

    def copy(n):
        start = pl.multiple_of(spots[n] // 8 * 8, 8)
        return pltpu.make_async_copy(prior.at[pl.ds(start, 8), :], tiles.at[n], arrive)

    def begin(n, carry):
        copy(n).start()
        return carry

    lax.fori_loop(0, found, begin, 0)
    total[...] = jnp.zeros_like(total)

    def finish(n, carry):
        copy(n).wait()
        return carry

    lax.fori_loop(0, found, finish, 0)

    def place(n, carry):
        tile = tiles[n].astype(jnp.float32)
        at = lax.broadcasted_iota(jnp.int32, tile.shape, 0)
        row = jnp.sum(jnp.where(at == spots[n] % 8, tile, 0.0), axis=0, keepdims=True)
        total[pl.ds(owned[n], 1), :] = row
        return carry

    lax.fori_loop(0, found, place, 0)
    half = count // cores
    c = me[0] % cores
    kept[...] = total[pl.ds(pl.multiple_of(c * half, 8), half), :].astype(kept.dtype)
    if cores > 1:
        sent[...] = total[pl.ds(pl.multiple_of((1 - c) * half, 8), half), :].astype(sent.dtype)


def pick(pivots, me, prior, cores):
    count = pivots.shape[0]
    width = prior.shape[1]
    shape = jax.ShapeDtypeStruct((count // cores, width), prior.dtype)
    return call(
        functools.partial(pick_kernel, cores=cores),
        [shape, shape],
        [pivots, me, keep(prior)],
        [SMEM, SMEM, HBM],
        [VMEM, VMEM],
        scratch=[
            pltpu.VMEM((count, 8, width), prior.dtype),
            pltpu.VMEM((count, width), jnp.float32),
            pltpu.SMEM((count + 8,), jnp.int32),
            pltpu.SMEM((count + 8,), jnp.int32),
            pltpu.SemaphoreType.DMA,
        ],
        limit=5,
    )


def parts_kernel(me, mine, *rest, cores, groups):
    prior, kept = rest[0], rest[1]
    outs = rest[1 + cores : 1 + cores + groups]
    picked = rest[-1]
    height = outs[0].shape[0]
    half = kept.shape[0]
    c = me[0] % cores
    picked[pl.ds(pl.multiple_of(c * half, 8), half), :] = kept[...]
    if cores > 1:
        picked[pl.ds(pl.multiple_of((1 - c) * half, 8), half), :] = rest[2][...]
    for g in range(groups):
        start = (mine[0] + 1 + g) % groups * height
        outs[g][...] = lax.dot_general(
            prior[pl.ds(pl.multiple_of(start, 8), height), :],
            picked[...],
            (((1,), (1,)), ((), ())),
            preferred_element_type=jnp.float32,
        ).astype(outs[g].dtype)


def parts_of(me, mine, prior, picked, cores, groups):
    rows, width = prior.shape
    count = picked[0].shape[0] * cores
    height = rows // groups
    return call(
        functools.partial(parts_kernel, cores=cores, groups=groups),
        [jax.ShapeDtypeStruct((height, count), prior.dtype)] * groups,
        [me, mine, prior, *picked],
        [SMEM, SMEM, VMEM] + [VMEM] * cores,
        [VMEM] * groups,
        scratch=[pltpu.VMEM((count, width), prior.dtype)],
        limit=16,
    )


def local(old_block, vectors, prior, pair_columns, pivots):
    size = lax.axis_size("gx")
    groups = lax.axis_size("gy")
    far, near, cores = factors(size)
    me = lax.axis_index("gx")
    mine = lax.axis_index("gy")
    everyone = [(a, b, d) for a in range(far) for b in range(near) for d in range(cores)]

    def place(a, b, d):
        return (a % far * near + b % near) * cores + d % cores

    def shift(x, a=0, b=0, d=0):
        return lax.ppermute(x, "gx", [(place(i, j, k), place(i + a, j + b, k + d)) for i, j, k in everyone])

    def swap_far(x, bit):
        return lax.ppermute(x, "gx", [(place(i, j, k), place(i ^ bit, j, k)) for i, j, k in everyone])

    own = vectors.reshape(vectors.shape[0], vectors.shape[2])
    width = own.shape[1]
    tiled = width % 128 == 0

    lines = [(own, 0)]
    forward = backward = own
    if tiled:
        for step in range(1, far // 2 + 1):
            forward = shift(forward, a=1)
            lines.append((forward, -step))
            if step < far - far // 2:
                backward = shift(backward, a=-1)
                lines.append((backward, step))

    slab = own
    reach = 1
    while reach < groups:
        got = lax.ppermute(slab, "gy", [(g, (g + reach) % groups) for g in range(groups)])
        takes = jnp.logical_and(mine >= reach, mine < 2 * reach)
        reach *= 2
        if reach < groups:
            slab = jnp.where(takes, got, slab)
    if groups == 1:
        got, takes = own, mine > 0
    if groups > 2:
        got, takes = jnp.where(takes, got, slab), mine >= 0

    kept, sent = pick(pivots, me[None], prior, cores)

    if tiled:
        blocks, spots = {}, {}
        for line, (block, away) in enumerate(lines):
            at = line * near * cores
            blocks[at] = block
            for e in range(near):
                for f in range(cores):
                    spots[at + e * cores + f] = (away, e, f)
            if cores > 1:
                blocks[at + 1] = shift(block, d=1)
            if near > 1:
                blocks[at + cores] = shift(block, b=1)
                if cores > 1:
                    blocks[at + cores + 1] = shift(blocks[at + cores], d=1)

    if cores > 1:
        kept = add(kept, shift(sent, d=1))
    if near > 1:
        kept = add(kept, shift(kept, b=1))
    bit = 1
    while bit < far:
        kept = add(kept, swap_far(kept, bit))
        bit *= 2
    picked = [kept]
    if cores > 1:
        picked.append(shift(kept, d=1))

    parts = parts_of(me[None], mine[None], prior, picked, cores, groups)
    arrived = []
    for step in range(1, groups):
        arrived.append(lax.ppermute(parts[step - 1], "gy", [(g, (g + step) % groups) for g in range(groups)]))

    if tiled:
        new_block = None
        order = batches(far, near, cores)
        rows_of = (takes.astype(jnp.int32)[None], got)
        for number, batch in enumerate(order):
            done = update(
                me[None],
                rows_of,
                old_block,
                [blocks[at] for at in batch],
                [spots[at] for at in batch],
                (far, near, cores),
                new_block,
                (pair_columns, parts[-1], *arrived) if batch == order[-1] else (),
            )
            new_block = done[0]
            if number == 0:
                rows_of = done[1]
        return new_block, done[1]

    every = lax.all_gather(own, "gx", axis=1, tiled=True)
    slab = jnp.where(takes, got, slab)
    new_block = old_block + jnp.dot(slab.T, every, preferred_element_type=jnp.float32)
    total = parts[-1].astype(jnp.float32)
    for part in arrived:
        total = total + part.astype(jnp.float32)
    return new_block, pair_columns - total


def batches(far, near, cores):
    if (far, near, cores) == (4, 2, 2):
        return [[0, 1], [2, 3, 4, 5], [6, 7, 12, 13], [14, 15, 8, 9], [10, 11]]
    return [list(range(at, at + near * cores)) for at in range(0, far * near * cores, near * cores)]


def solution(mesh):
    placed = (P("gx", "gy"), P(None, "gy", "gx"), P("gx", "gy"), P(("gx", "gy"), None), P())

    return jax.shard_map(
        local,
        mesh=mesh,
        in_specs=placed,
        out_specs=(P("gx", "gy"), P(("gx", "gy"), None)),
        check_vma=False,
    )
```

```python
import functools

import jax
import jax.numpy as jnp
from jax import lax
from jax.experimental import pallas as pl
from jax.experimental.pallas import tpu as pltpu
from jax.sharding import PartitionSpec as P


def factors(n):
    core = 2 if n % 2 == 0 else 1
    near = 2 if (n // core) % 2 == 0 else 1
    return n // (core * near), near, core


HELD = 0
HBM = pl.BlockSpec(memory_space=pltpu.HBM)
VMEM = pl.BlockSpec(memory_space=pltpu.VMEM)
SMEM = pl.BlockSpec(memory_space=pltpu.SMEM)


def keep(x):
    return pltpu.with_memory_space_constraint(x, pltpu.HBM)


def call(kernel, out_shape, operands, specs, out_specs, scratch=(), aliases=None, limit=8, flops=0):
    return pl.pallas_call(
        kernel,
        out_shape=out_shape,
        in_specs=specs,
        out_specs=out_specs,
        scratch_shapes=list(scratch),
        input_output_aliases=aliases or {},
        compiler_params=pltpu.CompilerParams(vmem_limit_bytes=limit * 1024 * 1024),
        cost_estimate=pl.CostEstimate(flops=flops, bytes_accessed=0, transcendentals=0),
    )(*operands)


def window(me, spots, extent, high, width):
    far, near, cores = extent
    z, y, c = me[0] // (near * cores), me[0] // cores % near, me[0] % cores

    def spot(at, tile):
        a, b, d = spots[at]
        column = (((z + a + far) % far * near) + (y + b) % near) * cores + (c + d) % cores
        return pl.ds(tile * high, high), pl.ds(pl.multiple_of(column * width, 128), width)

    return spot


def hold_kernel(me, own, old, before, mine, arrive, here, *, spots, extent, tiles):
    high, width = before.shape[1:]
    spot = window(me, spots, extent, high, width)
    copies = [pltpu.make_async_copy(own, mine, here)]
    for n in range(len(spots) * tiles):
        copies.append(pltpu.make_async_copy(old.at[spot(n // tiles, n % tiles)], before.at[n], arrive.at[n]))
    for copy in copies:
        copy.start()
    for copy in copies:
        copy.wait()


def row_tiles(rows):
    return next(t for t in (2, 1) if rows % (8 * t) == 0)


def hold(me, own, old, spots, extent):
    tiles = row_tiles(old.shape[0])
    count = len(spots) * tiles
    return call(
        functools.partial(hold_kernel, spots=spots, extent=extent, tiles=tiles),
        [
            jax.ShapeDtypeStruct((count, old.shape[0] // tiles, own.shape[1]), old.dtype),
            jax.ShapeDtypeStruct(own.shape, own.dtype),
        ],
        [me, keep(own), keep(old)],
        [SMEM, HBM, HBM],
        [VMEM, VMEM],
        scratch=[pltpu.SemaphoreType.DMA((count,)), pltpu.SemaphoreType.DMA],
    )


def update_kernel(me, *rest, spots, extent, tiles, first, tail, ready, skip):
    count = len(spots)
    if tail:
        rest, (total, pair_in, pair_out) = rest[:-3], rest[-3:]
    held, arrive, leave = rest[-3:]
    high, width = held.shape[1:]
    pieces = [(at, tile) for at in range(count) for tile in range(tiles)]
    lag = 3 if len(pieces) >= 8 else 0
    spot = window(me, spots, extent, high, width)
    if ready:
        before, rest = rest[0], rest[1:]
    if first:
        mask, got, *blocks = rest[: count + 2]
        old, out, slab = rest[count + 2 : count + 5]
    else:
        slab, *blocks = rest[: count + 1]
        old = rest[count + 1]
        pair, *parts = rest[count + 3 : count + 3 + tail] if tail else [None]
        out = rest[count + 3 + tail]

    def load(n):
        return pltpu.make_async_copy(old.at[spot(*pieces[n])], held.at[n], arrive.at[n])

    def save(n):
        return pltpu.make_async_copy(held.at[n], out.at[spot(*pieces[n])], leave.at[n])

    for n in range(ready, len(pieces)):
        load(n).start()
    if tail:
        residual = rest[count + 4 + tail]
        pair_load = pltpu.make_async_copy(pair, total, pair_in)
        pair_save = pltpu.make_async_copy(total, residual, pair_out)
        pair_load.start()
    if first:
        chosen = jnp.where(mask[0] != 0, got[...].astype(jnp.float32), blocks[0][...].astype(jnp.float32))
        slab[...] = chosen.T.astype(slab.dtype)
    for n, (at, tile) in enumerate(pieces):
        if n >= ready:
            load(n).wait()
        start = before[skip + n] if n < ready else held[n]
        held[n] = start + jnp.dot(
            slab[tile * high : (tile + 1) * high, :], blocks[at][...], preferred_element_type=jnp.float32
        )
        if n >= lag:
            save(n - lag).start()
    if tail:
        pair_load.wait()
        gathered = parts[0][...].astype(jnp.float32)
        for part in parts[1:]:
            gathered = gathered + part[...].astype(jnp.float32)
        total[...] -= gathered
        pair_save.start()
    for n in range(len(pieces) - lag, len(pieces)):
        save(n).start()
    if tail:
        pair_save.wait()
    for n in range(len(pieces)):
        save(n).wait()


def update(me, rows_of, old, blocks, spots, extent, target, tail=(), before=None, ready=0, skip=0):
    first = target is None
    inner, width = blocks[-1].shape
    rows = old.shape[0]
    count = len(blocks)
    tiles = row_tiles(rows)
    high = rows // tiles
    early = [before] if ready else []
    shape = jax.ShapeDtypeStruct(old.shape, old.dtype)
    scratch = [
        pltpu.VMEM((count * tiles, high, width), old.dtype),
        pltpu.SemaphoreType.DMA((count * tiles,)),
        pltpu.SemaphoreType.DMA((count * tiles,)),
    ]
    if first:
        mask, got = rows_of
        operands = [me, *early, mask, got, *blocks, keep(old)]
        specs = [SMEM] + [VMEM] * len(early) + [SMEM, VMEM] + [VMEM] * count + [HBM]
        aliases = {}
        outs = [shape, jax.ShapeDtypeStruct((rows, inner), got.dtype)]
        out_specs = [HBM, VMEM]
    else:
        operands = [me, *early, rows_of, *blocks, keep(old), target]
        specs = [SMEM] + [VMEM] * len(early) + [VMEM] + [VMEM] * count + [HBM, HBM]
        aliases = {len(operands) - 1: 0}
        outs, out_specs = [shape], [HBM]
        if tail:
            operands += [keep(tail[0]), *tail[1:]]
            specs += [HBM] + [VMEM] * (len(tail) - 1)
            outs.append(jax.ShapeDtypeStruct(tail[0].shape, tail[0].dtype))
            out_specs.append(HBM)
            scratch += [
                pltpu.VMEM(tail[0].shape, tail[0].dtype),
                pltpu.SemaphoreType.DMA,
                pltpu.SemaphoreType.DMA,
            ]
    return call(
        functools.partial(update_kernel, spots=spots, extent=extent, tiles=tiles, first=first, tail=len(tail), ready=ready * tiles, skip=skip * tiles),
        outs,
        operands,
        specs,
        out_specs,
        scratch=scratch,
        aliases=aliases,
        limit=16,
        flops=2 * rows * inner * width * count,
    )


def add_kernel(a, b, out):
    out[...] = a[...] + b[...]


def add(a, b):
    return call(add_kernel, jax.ShapeDtypeStruct(a.shape, a.dtype), [a, b], [VMEM, VMEM], VMEM)


def pick_kernel(pivots, me, prior, kept, sent, tiles, total, owned, spots, arrive, *, cores):
    count = pivots.shape[0]
    rows = prior.shape[0]
    base = me[0] * rows

    def list_owned(k, found):
        row = pivots[k] - base
        owned[found] = k
        spots[found] = row
        return found + jnp.where(jnp.logical_and(row >= 0, row < rows), 1, 0)

    found = lax.fori_loop(0, count, list_owned, 0, unroll=8)

    def copy(n):
        start = pl.multiple_of(spots[n] // 8 * 8, 8)
        return pltpu.make_async_copy(prior.at[pl.ds(start, 8), :], tiles.at[n], arrive)

    def begin(n, carry):
        copy(n).start()
        return carry

    lax.fori_loop(0, found, begin, 0)
    total[...] = jnp.zeros_like(total)

    def finish(n, carry):
        copy(n).wait()
        return carry

    lax.fori_loop(0, found, finish, 0)

    def place(n, carry):
        tile = tiles[n].astype(jnp.float32)
        at = lax.broadcasted_iota(jnp.int32, tile.shape, 0)
        row = jnp.sum(jnp.where(at == spots[n] % 8, tile, 0.0), axis=0, keepdims=True)
        total[pl.ds(owned[n], 1), :] = row
        return carry

    lax.fori_loop(0, found, place, 0)
    half = count // cores
    c = me[0] % cores
    kept[...] = total[pl.ds(pl.multiple_of(c * half, 8), half), :].astype(kept.dtype)
    if cores > 1:
        sent[...] = total[pl.ds(pl.multiple_of((1 - c) * half, 8), half), :].astype(sent.dtype)


def pick(pivots, me, prior, cores):
    count = pivots.shape[0]
    width = prior.shape[1]
    shape = jax.ShapeDtypeStruct((count // cores, width), prior.dtype)
    return call(
        functools.partial(pick_kernel, cores=cores),
        [shape, shape],
        [pivots, me, keep(prior)],
        [SMEM, SMEM, HBM],
        [VMEM, VMEM],
        scratch=[
            pltpu.VMEM((count, 8, width), prior.dtype),
            pltpu.VMEM((count, width), jnp.float32),
            pltpu.SMEM((count + 8,), jnp.int32),
            pltpu.SMEM((count + 8,), jnp.int32),
            pltpu.SemaphoreType.DMA,
        ],
        limit=5,
    )


def parts_kernel(me, mine, *rest, cores, groups):
    prior, kept = rest[0], rest[1]
    outs = rest[1 + cores : 1 + cores + groups]
    picked = rest[-1]
    height = outs[0].shape[0]
    half = kept.shape[0]
    c = me[0] % cores
    picked[pl.ds(pl.multiple_of(c * half, 8), half), :] = kept[...]
    if cores > 1:
        picked[pl.ds(pl.multiple_of((1 - c) * half, 8), half), :] = rest[2][...]
    for g in range(groups):
        start = (mine[0] + 1 + g) % groups * height
        outs[g][...] = lax.dot_general(
            prior[pl.ds(pl.multiple_of(start, 8), height), :],
            picked[...],
            (((1,), (1,)), ((), ())),
            preferred_element_type=jnp.float32,
        ).astype(outs[g].dtype)


def parts_of(me, mine, prior, picked, cores, groups):
    rows, width = prior.shape
    count = picked[0].shape[0] * cores
    height = rows // groups
    return call(
        functools.partial(parts_kernel, cores=cores, groups=groups),
        [jax.ShapeDtypeStruct((height, count), prior.dtype)] * groups,
        [me, mine, prior, *picked],
        [SMEM, SMEM, VMEM] + [VMEM] * cores,
        [VMEM] * groups,
        scratch=[pltpu.VMEM((count, width), prior.dtype)],
        limit=16,
    )


def local(old_block, vectors, prior, pair_columns, pivots):
    size = lax.axis_size("gx")
    groups = lax.axis_size("gy")
    far, near, cores = factors(size)
    me = lax.axis_index("gx")
    mine = lax.axis_index("gy")
    everyone = [(a, b, d) for a in range(far) for b in range(near) for d in range(cores)]

    def place(a, b, d):
        return (a % far * near + b % near) * cores + d % cores

    def shift(x, a=0, b=0, d=0):
        return lax.ppermute(x, "gx", [(place(i, j, k), place(i + a, j + b, k + d)) for i, j, k in everyone])

    def swap_far(x, bit):
        return lax.ppermute(x, "gx", [(place(i, j, k), place(i ^ bit, j, k)) for i, j, k in everyone])

    own = vectors.reshape(vectors.shape[0], vectors.shape[2])
    width = own.shape[1]
    tiled = width % 128 == 0

    lines = [(own, 0)]
    forward = backward = own
    if tiled:
        for step in range(1, far // 2 + 1):
            forward = shift(forward, a=1)
            lines.append((forward, -step))
            if step < far - far // 2:
                backward = shift(backward, a=-1)
                lines.append((backward, step))

    slab = own
    reach = 1
    while reach < groups:
        got = lax.ppermute(slab, "gy", [(g, (g + reach) % groups) for g in range(groups)])
        takes = jnp.logical_and(mine >= reach, mine < 2 * reach)
        reach *= 2
        if reach < groups:
            slab = jnp.where(takes, got, slab)
    if groups == 1:
        got, takes = own, mine > 0
    if groups > 2:
        got, takes = jnp.where(takes, got, slab), mine >= 0

    kept, sent = pick(pivots, me[None], prior, cores)

    if tiled:
        blocks, spots = {}, {}
        for line, (block, away) in enumerate(lines):
            at = line * near * cores
            blocks[at] = block
            for e in range(near):
                for f in range(cores):
                    spots[at + e * cores + f] = (away, e, f)
            if cores > 1:
                blocks[at + 1] = shift(block, d=1)
            if near > 1:
                blocks[at + cores] = shift(block, b=1)
                if cores > 1:
                    blocks[at + cores + 1] = shift(blocks[at + cores], d=1)

    if cores > 1:
        kept = add(kept, shift(sent, d=1))
    if near > 1:
        kept = add(kept, shift(kept, b=1))
    bit = 1
    while bit < far:
        kept = add(kept, swap_far(kept, bit))
        bit *= 2
    picked = [kept]
    if cores > 1:
        picked.append(shift(kept, d=1))

    parts = parts_of(me[None], mine[None], prior, picked, cores, groups)
    arrived = []
    for step in range(1, groups):
        arrived.append(lax.ppermute(parts[step - 1], "gy", [(g, (g + step) % groups) for g in range(groups)]))

    if tiled:
        new_block = None
        order = batches(far, near, cores)
        rows_of = (takes.astype(jnp.int32)[None], got)
        early = order[0] + order[1][:HELD]
        before, blocks[0] = hold(me[None], own, old_block, [spots[at] for at in early], (far, near, cores))
        for number, batch in enumerate(order):
            done = update(
                me[None],
                rows_of,
                old_block,
                [blocks[at] for at in batch],
                [spots[at] for at in batch],
                (far, near, cores),
                new_block,
                (pair_columns, parts[-1], *arrived) if batch == order[-1] else (),
                before,
                (len(order[0]), min(HELD, len(order[1])))[number] if number < 2 else 0,
                len(order[0]) * number,
            )
            new_block = done[0]
            if number == 0:
                rows_of = done[1]
        return new_block, done[1]

    every = lax.all_gather(own, "gx", axis=1, tiled=True)
    slab = jnp.where(takes, got, slab)
    new_block = old_block + jnp.dot(slab.T, every, preferred_element_type=jnp.float32)
    total = parts[-1].astype(jnp.float32)
    for part in arrived:
        total = total + part.astype(jnp.float32)
    return new_block, pair_columns - total


def batches(far, near, cores):
    if (far, near, cores) == (4, 2, 2):
        return [[0, 1], [2, 3, 4, 5], [6, 7, 12, 13], [14, 15, 8, 9], [10, 11]]
    return [list(range(at, at + near * cores)) for at in range(0, far * near * cores, near * cores)]


def solution(mesh):
    placed = (P("gx", "gy"), P(None, "gy", "gx"), P("gx", "gy"), P(("gx", "gy"), None), P())

    return jax.shard_map(
        local,
        mesh=mesh,
        in_specs=placed,
        out_specs=(P("gx", "gy"), P(("gx", "gy"), None)),
        check_vma=False,
    )
```
